256 devices in a mesh: expert: 16 (over x, y), tensor: 8 (over z), replica: 2 (over core).
Axes of the slice: x: 4, y: 4, z: 8, core: 2. Of those that a mesh axis runs over, the one named last changes fastest.
Arguments:
- trained: float32 [16, 7168, 2048], P('replica', 'tensor', 'expert'), may hold values from -3080 to 3080
- snapshot: bfloat16 [16, 7168, 2048], P('replica', 'tensor', 'expert'), may hold values from -3072 to 3072
- changed: int32 [16, 56, 16], P('replica', 'tensor', 'expert'), may hold values from 0 to 1, as said below
- placement: int32 [16], replicated, may hold values from 0 to 15, each once
Outputs:
- rotated_update: bfloat16 [16, 7168, 2048], P('expert', None, 'tensor')
The draws below stay inside these ranges and needn't reach their ends.
Inputs may be any that keep to these rules, and one draw needn't show every extreme that they name: `placement`: each of the 16 experts appears exactly once. `changed`: in each aligned block of 7 block rows by 1 block columns of one expert, at most 4 entries are 1; for every expert some such block has exactly 4.
All inputs are finite; a program needn't handle non-finite values.
Results may differ from the reference program's by a relative error of at most 0.001.
Values may be sent and summed in bfloat16 or wider, within the bound.
A program may use at most 64 MiB of HBM per device.

```python
import math
import jax
import jax.numpy as jnp
from jax import lax

D = 7168
FF = 2048
BLK = 128
E = 16
RB = 56
CB = 16
RBT = 7
CBE = 1
MOST = 4


def log_uniform(key, shape, low, high):
    return jnp.exp(jax.random.uniform(key, shape, jnp.float32, math.log(low), math.log(high)))


def draw_changed(key, part):
    tensor_groups = D // (BLK * RBT)
    expert_groups = FF // (BLK * CBE)
    group_count = tensor_groups * expert_groups
    block_count = RBT * CBE
    key_counts, key_forced, key_order = jax.random.split(jax.random.fold_in(key, 7), 3)
    counts = jax.random.randint(key_counts, (E, group_count), 0, MOST + 1)
    forced = jax.random.randint(key_forced, (E,), 0, group_count)
    counts = jnp.where(jnp.arange(group_count)[None, :] == forced[:, None], MOST, counts)
    scores = jax.random.randint(key_order, (E, group_count, block_count), 0, 1 << 16) * block_count
    scores = scores + jnp.arange(block_count, dtype=jnp.int32)[None, None, :]
    rank_ids = jnp.argsort(jnp.argsort(scores, axis=2), axis=2)
    chosen_mask = (rank_ids < counts[:, :, None]).astype(jnp.int32)
    chosen_mask = chosen_mask.reshape(E, tensor_groups, expert_groups, RBT, CBE)
    chosen_mask = jnp.transpose(chosen_mask, (0, 1, 3, 2, 4))
    return chosen_mask.reshape(E, tensor_groups * RBT, expert_groups * CBE)


def base_values(key):
    key_base = jax.random.fold_in(key, 11)
    return 512.0 * jnp.clip(jax.random.normal(key_base, (E, D, FF), jnp.float32), -6.0, 6.0)


def draw_snapshot(key, part):
    return base_values(key).astype(jnp.bfloat16)


def draw_trained(key, part):
    anchor = base_values(key).astype(jnp.bfloat16).astype(jnp.float32)
    block_flags = draw_changed(key, part)
    key_large, key_small, key_jitter = jax.random.split(jax.random.fold_in(key, 23), 3)
    large_scale = log_uniform(key_large, (E, RB, CB), 0.25, 1.0)
    jitter = jnp.clip(jax.random.normal(key_jitter, (E, D, FF), jnp.float32), -6.0, 6.0)
    small_scale = log_uniform(key_small, (E, RB, CB), 0.04, 0.12)
    scales = jnp.where(block_flags == 1, large_scale, small_scale)
    jitter = jitter.reshape(E, RB, BLK, CB, BLK) * scales[:, :, None, :, None]
    return anchor + jitter.reshape(E, D, FF)


def setup_inputs(seed: int = 0) -> dict:
    key_of = jax.random.split(jax.random.key(seed), 5)
    return {
        "trained": draw_trained(jax.random.fold_in(key_of[4], 71), 0),
        "snapshot": draw_snapshot(jax.random.fold_in(key_of[4], 71), 0),
        "changed": draw_changed(jax.random.fold_in(key_of[4], 71), 0),
        "placement": jax.random.permutation(key_of[3], E).astype(jnp.int32),
    }


def hadamard():
    positions = jnp.arange(BLK, dtype=jnp.int32)
    parity = jnp.zeros((BLK, BLK), jnp.int32)
    for bit_level in range(BLK.bit_length() - 1):
        parity = parity + (positions[:, None] >> bit_level & 1) * (positions[None, :] >> bit_level & 1)
    return (1 - 2 * (parity % 2)).astype(jnp.float32) / math.sqrt(BLK)

def reference(trained, snapshot, changed, placement):
    hadamard_table = hadamard()

    def one_slot(expert):
        newest = trained[expert]
        previous = snapshot[expert].astype(jnp.float32)
        block_flags = changed[expert]
        delta_grid = (newest - previous).reshape(RB, BLK, CB, BLK)
        delta_grid = jnp.where(block_flags[:, None, :, None] == 1, delta_grid, 0.0).reshape(RB, BLK, FF)
        coded_grid = jnp.einsum('ij,ajc->aic', hadamard_table, delta_grid, precision=lax.Precision.HIGHEST)
        return coded_grid.reshape(D, FF).astype(jnp.bfloat16)
    return lax.map(one_slot, placement)
```

```python
import math

import jax
import jax.numpy as jnp
from jax import lax
from jax.experimental import pallas as pl
from jax.experimental.pallas import tpu as pltpu
from jax.sharding import PartitionSpec as P

MESH = pl.DeviceIdType.MESH
BLK = 128
MOST = 4
HALF = MOST // 2
META = 16
ROWS = HALF * BLK + META


def sign_table(rows, cols):
    shared = lax.broadcasted_iota(jnp.int32, (rows, cols), 0) & (
        lax.broadcasted_iota(jnp.int32, (rows, cols), 1) & (BLK - 1)
    )
    shared = shared ^ (shared >> 4)
    shared = shared ^ (shared >> 2)
    shared = shared ^ (shared >> 1)
    return (1 - 2 * (shared & 1)).astype(jnp.float32).astype(jnp.bfloat16)


def push_kernel(sizes, trained, snapshot, changed, placement, result, new_bufs, old_bufs, table, mine, other, staged, passing, sems):
    expert_count, tensor_count, local_experts, block_rows = sizes
    (in_sem, swap_send, swap_recv, plane_send, plane_recv, z_send, z_recv, last_send, last_recv) = sems
    c = lax.axis_index("expert")
    z = lax.axis_index("tensor")
    r = lax.axis_index("replica")
    slots = expert_count
    group = expert_count // tensor_count

    barrier = pltpu.get_barrier_semaphore()

    pl.semaphore_signal(barrier, inc=1, device_id=(c, z, 1 - r), device_id_type=MESH)

    @pl.loop(1, expert_count)
    def _(step):
        pl.semaphore_signal(barrier, inc=1, device_id=(lax.rem(c + step, expert_count), z, r), device_id_type=MESH)

    @pl.loop(1, tensor_count)
    def _(step):
        pl.semaphore_signal(barrier, inc=1, device_id=(c, lax.rem(z + step, tensor_count), r), device_id_type=MESH)

    def loads(e):
        return (
            pltpu.make_async_copy(trained.at[e], new_bufs[e], in_sem.at[0, e]),
            pltpu.make_async_copy(snapshot.at[e], old_bufs[e], in_sem.at[1, e]),
        )

    for e in range(local_experts):
        for load in loads(e):
            load.start()

    table[...] = sign_table(BLK, 2 * BLK)
    pl.semaphore_wait(barrier, expert_count + tensor_count - 1)

    def swap(e):
        return pltpu.make_async_remote_copy(
            src_ref=other.at[e],
            dst_ref=mine.at[r * local_experts + e],
            send_sem=swap_send.at[e],
            recv_sem=swap_recv.at[e],
            device_id=(c, z, 1 - r),
            device_id_type=MESH,
        )

    row_ids = lax.broadcasted_iota(jnp.int32, (META, BLK), 0)

    for e in range(local_experts):
        for load in loads(e):
            load.wait()
        count = jnp.int32(0)
        spots = [jnp.int32(block_rows)] * MOST
        picks = [jnp.int32(0)] * MOST
        for b in range(block_rows):
            flag = changed[e, b]
            for k in range(MOST):
                hit = (flag == 1) & (count == k)
                spots[k] = jnp.where(hit, b, spots[k])
                picks[k] = jnp.where(hit, b, picks[k])
            count = count + flag
        highs, lows = [], []
        for k in range(MOST):
            delta = new_bufs[e][picks[k]] - old_bufs[e][picks[k]].astype(jnp.float32)
            high = delta.astype(jnp.bfloat16)
            highs.append(high)
            lows.append((delta - high.astype(jnp.float32)).astype(jnp.bfloat16))
        parts = jnp.concatenate([jnp.concatenate(highs, axis=1), jnp.concatenate(lows, axis=1)], axis=0)
        coded = jnp.dot(table[...], parts, preferred_element_type=jnp.float32) * (1.0 / math.sqrt(BLK))
        coded = coded.astype(jnp.bfloat16)

        def store(ref, index, first, coded=coded, spots=spots):
            for k in range(HALF):
                ref[index, k * BLK : (k + 1) * BLK, :] = coded[:, (first + k) * BLK : (first + k + 1) * BLK]
            spot = jnp.where(row_ids < META // 2, spots[first], spots[first + 1])
            ref[index, HALF * BLK : ROWS, :] = spot.astype(jnp.float32).astype(jnp.bfloat16)

        own = r * local_experts + e

        @pl.when(r == 0)
        def _():
            store(mine, own, 0)
            store(other, e, HALF)

        @pl.when(r == 1)
        def _():
            store(mine, own, HALF)
            store(other, e, 0)

        if e > 0:
            swap(e - 1).start()

    swap(local_experts - 1).start()

    @pl.loop(0, local_experts)
    def _(e):
        swap(e).wait_recv()

    home = c // group == z

    @pl.when(home)
    def _():
        result[r, c] = mine[placement[c]]

    @pl.when(jnp.logical_not(home))
    def _():
        passing[c] = mine[placement[c]]

    spot_here = z * group + lax.rem(c, group)

    def plane(s):
        return pltpu.make_async_remote_copy(
            src_ref=staged.at[s],
            dst_ref=passing.at[c],
            send_sem=plane_send.at[s],
            recv_sem=plane_recv.at[c],
            device_id=(s, z, r),
            device_id_type=MESH,
        )

    def plane_home(s):
        return pltpu.make_async_remote_copy(
            src_ref=staged.at[s],
            dst_ref=result.at[r, spot_here],
            send_sem=plane_send.at[s],
            recv_sem=z_recv.at[spot_here],
            device_id=(s, z, r),
            device_id_type=MESH,
        )

    def shift(step):
        turn = lax.rem(step, 2) * (slots // 2) + step // 2
        return lax.rem(turn + group * z, slots)

    @pl.loop(0, slots)
    def _(step):
        s = lax.rem(c + slots - shift(step), slots)

        @pl.when(s != c)
        def _():
            staged[s] = mine[placement[s]]

            @pl.when(home)
            def _():
                plane_home(s).start()

            @pl.when(jnp.logical_not(home))
            def _():
                plane(s).start()

    def along(source):
        spot = z * group + lax.rem(source, group)
        return pltpu.make_async_remote_copy(
            src_ref=passing.at[source],
            dst_ref=result.at[r, spot],
            send_sem=z_send.at[source],
            recv_sem=z_recv.at[spot],
            device_id=(c, source // group, r),
            device_id_type=MESH,
        )

    def plane_from(source):
        return pltpu.make_async_remote_copy(
            src_ref=staged.at[source],
            dst_ref=passing.at[source],
            send_sem=plane_send.at[source],
            recv_sem=plane_recv.at[source],
            device_id=(source, z, r),
            device_id_type=MESH,
        )

    @pl.loop(0, slots)
    def _(step):
        source = lax.rem(c + shift(step), slots)

        @pl.when(source // group != z)
        def _():
            @pl.when(source != c)
            def _():
                plane_from(source).wait_recv()

            along(source).start()

    def last(spot):
        return pltpu.make_async_remote_copy(
            src_ref=result.at[r, spot],
            dst_ref=result.at[r, spot],
            send_sem=last_send.at[spot],
            recv_sem=last_recv.at[spot],
            device_id=(c, z, 1 - r),
            device_id_type=MESH,
        )

    def arrived(spot):
        return pltpu.make_async_remote_copy(
            src_ref=result.at[r, spot],
            dst_ref=result.at[r, spot],
            send_sem=z_send.at[spot],
            recv_sem=z_recv.at[spot],
            device_id=(c, z, 1 - r),
            device_id_type=MESH,
        )

    def last_from(spot):
        return pltpu.make_async_remote_copy(
            src_ref=result.at[1 - r, spot],
            dst_ref=result.at[1 - r, spot],
            send_sem=last_send.at[spot],
            recv_sem=last_recv.at[spot],
            device_id=(c, z, 1 - r),
            device_id_type=MESH,
        )

    @pl.loop(0, slots)
    def _(step):
        turn = lax.rem(step, 2) * (slots // 2) + step // 2
        spot = lax.rem(z * group + slots - turn, slots)

        @pl.when(jnp.logical_not(home & (spot == c)))
        def _():
            arrived(spot).wait_recv()

        last(spot).start()

    @pl.loop(0, local_experts)
    def _(e):
        swap(e).wait_send()

    @pl.loop(0, slots)
    def _(s):
        @pl.when(s != c)
        def _():
            plane(s).wait_send()

        @pl.when(s // group != z)
        def _():
            along(s).wait_send()

        last(s).wait_send()
        last_from(s).wait_recv()


def push(trained, snapshot, changed, placement):
    local_experts, block_rows = changed.shape
    slots = placement.shape[0]
    sizes = (lax.axis_size("expert"), lax.axis_size("tensor"), local_experts, block_rows)
    dma = pltpu.SemaphoreType.DMA

    def kernel(a, b, c, d, result, *refs):
        new_bufs, old_bufs, refs = refs[:local_experts], refs[local_experts : 2 * local_experts], refs[2 * local_experts :]
        push_kernel(sizes, a, b, c, d, result, new_bufs, old_bufs, *refs[:5], refs[5:])

    return pl.pallas_call(
        kernel,
        name="push",
        out_shape=jax.ShapeDtypeStruct((2, slots, ROWS, BLK), jnp.bfloat16),
        in_specs=[
            pl.BlockSpec(memory_space=pltpu.HBM),
            pl.BlockSpec(memory_space=pltpu.HBM),
            pl.BlockSpec(memory_space=pltpu.SMEM),
            pl.BlockSpec(memory_space=pltpu.SMEM),
        ],
        out_specs=pl.BlockSpec(memory_space=pltpu.VMEM),
        scratch_shapes=[
            *[pltpu.VMEM(trained.shape[1:], jnp.float32) for _ in range(local_experts)],
            *[pltpu.VMEM(snapshot.shape[1:], jnp.bfloat16) for _ in range(local_experts)],
            pltpu.VMEM((BLK, 2 * BLK), jnp.bfloat16),
            pltpu.VMEM((slots, ROWS, BLK), jnp.bfloat16),
            pltpu.VMEM((local_experts, ROWS, BLK), jnp.bfloat16),
            pltpu.VMEM((slots, ROWS, BLK), jnp.bfloat16),
            pltpu.VMEM((slots, ROWS, BLK), jnp.bfloat16),
            dma((2, local_experts)),
            dma((local_experts,)),
            dma((local_experts,)),
            dma((slots,)),
            dma((slots,)),
            dma((slots,)),
            dma((slots,)),
            dma((slots,)),
            dma((slots,)),
        ],
        compiler_params=pltpu.CompilerParams(collective_id=0, has_side_effects=True, vmem_limit_bytes=60 * 1024 * 1024),
    )(trained, snapshot, changed, placement)


def spread_kernel(sizes, tiles, out, image, sems):
    tensor_count, group, block_rows = sizes

    def write(z):
        rows = pl.ds(pl.multiple_of(z * block_rows * BLK, BLK), block_rows * BLK)
        return pltpu.make_async_copy(image.at[z], out.at[0, rows, :], sems.at[z])

    @pl.loop(0, tensor_count)
    def _(z):
        for j in range(group):
            index = z * group + j
            spots = []
            for k in range(MOST):
                row = HALF * BLK + (k % HALF) * (META // HALF)
                spots.append(tiles[k // HALF, index, row : row + 1, :])
            chunk = 32
            for b in range(block_rows):
                masks = [jnp.broadcast_to(spots[k] == jnp.bfloat16(b), (chunk, BLK)) for k in range(MOST)]
                for first in range(0, BLK, chunk):
                    value = jnp.zeros((chunk, BLK), jnp.bfloat16)
                    for k in range(MOST):
                        row = (k % HALF) * BLK + first
                        value = jnp.where(masks[k], tiles[k // HALF, index, row : row + chunk, :], value)
                    image[z, b * BLK + first : b * BLK + first + chunk, j * BLK : (j + 1) * BLK] = value
        write(z).start()

    @pl.loop(0, tensor_count)
    def _(z):
        write(z).wait()


def spread(tiles, block_rows):
    tensor_count = lax.axis_size("tensor")
    group = tiles.shape[1] // tensor_count
    rows = block_rows * BLK

    def kernel(tiles_ref, out, image, sems):
        spread_kernel((tensor_count, group, block_rows), tiles_ref, out, image, sems)

    return pl.pallas_call(
        kernel,
        name="spread",
        out_shape=jax.ShapeDtypeStruct((1, tensor_count * rows, group * BLK), jnp.bfloat16),
        in_specs=[pl.BlockSpec(memory_space=pltpu.VMEM)],
        out_specs=pl.BlockSpec(memory_space=pl.ANY),
        scratch_shapes=[
            pltpu.VMEM((tensor_count, rows, group * BLK), jnp.bfloat16),
            pltpu.SemaphoreType.DMA((tensor_count,)),
        ],
        compiler_params=pltpu.CompilerParams(vmem_limit_bytes=24 * 1024 * 1024),
    )(tiles)


def body(trained, snapshot, changed, placement):
    local_experts, local_rows, _ = trained.shape
    block_rows = local_rows // BLK
    blocks = (local_experts, block_rows, BLK, BLK)
    tiles = push(trained.reshape(blocks), snapshot.reshape(blocks), changed.reshape(local_experts, block_rows), placement)
    return spread(tiles, block_rows)


def solution(mesh):
    in_specs = (
        P("replica", "tensor", "expert"),
        P("replica", "tensor", "expert"),
        P("replica", "tensor", "expert"),
        P(),
    )
    out_specs = P("expert", None, "tensor")
    return jax.shard_map(body, mesh=mesh, in_specs=in_specs, out_specs=out_specs, check_vma=False)
```

```python
import math

import jax
import jax.numpy as jnp
from jax import lax
from jax.experimental import pallas as pl
from jax.experimental.pallas import tpu as pltpu
from jax.sharding import PartitionSpec as P

MESH = pl.DeviceIdType.MESH
BLK = 128
MOST = 4
HALF = MOST // 2
META = 16
ROWS = HALF * BLK + META
BARRIER_AT = 4
AHEAD = 2
TURNS = (
    ((1, 0), (-1, 0), (0, 1), (0, -1), (2, 2)),
    ((1, 1), (-1, -1), (1, -1), (-1, 1)),
    ((2, 0), (1, 2), (-1, 2)),
    ((0, 2), (2, 1), (2, -1)),
)
WIDTH = max(len(turns) for turns in TURNS)


def sign_table(rows, cols):
    shared = lax.broadcasted_iota(jnp.int32, (rows, cols), 0) & (
        lax.broadcasted_iota(jnp.int32, (rows, cols), 1) & (BLK - 1)
    )
    shared = shared ^ (shared >> 4)
    shared = shared ^ (shared >> 2)
    shared = shared ^ (shared >> 1)
    return (1 - 2 * (shared & 1)).astype(jnp.float32).astype(jnp.bfloat16)


def push_kernel(
    sizes, trained, snapshot, changed_in, placement_in, result, new_bufs, old_bufs, changed, placement, table, mine, other, staged, passing, sems
):
    expert_count, tensor_count, local_experts, block_rows = sizes
    (in_sem, table_sem, swap_send, swap_recv, plane_send, plane_recv, z_send, z_recv, last_send, last_recv) = sems
    c = lax.axis_index("expert")
    z = lax.axis_index("tensor")
    r = lax.axis_index("replica")
    slots = expert_count
    group = expert_count // tensor_count
    side = math.isqrt(expert_count)

    small_loads = (
        pltpu.make_async_copy(changed_in, changed, table_sem.at[0]),
        pltpu.make_async_copy(placement_in, placement, table_sem.at[1]),
    )
    loads = [
        (
            pltpu.make_async_copy(trained.at[e], new_bufs[e], in_sem.at[0, e]),
            pltpu.make_async_copy(snapshot.at[e], old_bufs[e], in_sem.at[1, e]),
        )
        for e in range(local_experts)
    ]
    for load in small_loads:
        load.start()
    for pair in loads:
        for load in pair:
            load.start()

    barrier = pltpu.get_barrier_semaphore()

    pl.semaphore_signal(barrier, inc=1, device_id=(c, z, 1 - r), device_id_type=MESH)

    @pl.loop(1, expert_count)
    def _(step):
        pl.semaphore_signal(barrier, inc=1, device_id=(lax.rem(c + step, expert_count), z, r), device_id_type=MESH)

    @pl.loop(1, tensor_count)
    def _(step):
        pl.semaphore_signal(barrier, inc=1, device_id=(c, lax.rem(z + step, tensor_count), r), device_id_type=MESH)

    table[...] = sign_table(BLK, 2 * BLK)
    for load in small_loads:
        load.wait()

    def remote(src, dst, send_sem, recv_sem, device):
        return pltpu.make_async_remote_copy(
            src_ref=src, dst_ref=dst, send_sem=send_sem, recv_sem=recv_sem, device_id=device, device_id_type=MESH
        )

    def swap(e):
        return remote(other.at[e], mine.at[r * local_experts + e], swap_send.at[e], swap_recv.at[e], (c, z, 1 - r))

    row_ids = lax.broadcasted_iota(jnp.int32, (META, BLK), 0)

    for e in range(local_experts):
        count = jnp.int32(0)
        spots = [jnp.int32(block_rows)] * MOST
        picks = [jnp.int32(0)] * MOST
        for b in range(block_rows):
            flag = changed[b, 0, e]
            for k in range(MOST):
                hit = (flag == 1) & (count == k)
                spots[k] = jnp.where(hit, b, spots[k])
                picks[k] = jnp.where(hit, b, picks[k])
            count = count + flag
        for load in loads[e]:
            load.wait()
        highs, lows = [], []
        for k in range(MOST):
            delta = new_bufs[e][picks[k]] - old_bufs[e][picks[k]].astype(jnp.float32)
            high = delta.astype(jnp.bfloat16)
            highs.append(high)
            lows.append((delta - high.astype(jnp.float32)).astype(jnp.bfloat16))
        parts = jnp.concatenate([jnp.concatenate(highs, axis=1), jnp.concatenate(lows, axis=1)], axis=0)
        coded = jnp.dot(table[...], parts, preferred_element_type=jnp.float32) * (1.0 / math.sqrt(BLK))
        coded = coded.astype(jnp.bfloat16)

        def store(ref, index, first, coded=coded, spots=spots):
            for k in range(HALF):
                ref[index, k * BLK : (k + 1) * BLK, :] = coded[:, (first + k) * BLK : (first + k + 1) * BLK]
            spot = jnp.where(row_ids < META // 2, spots[first], spots[first + 1])
            ref[index, HALF * BLK : ROWS, :] = spot.astype(jnp.float32).astype(jnp.bfloat16)

        own = r * local_experts + e

        @pl.when(r == 0)
        def _():
            store(mine, own, 0)
            store(other, e, HALF)

        @pl.when(r == 1)
        def _():
            store(mine, own, HALF)
            store(other, e, 0)

        if e == BARRIER_AT:
            pl.semaphore_wait(barrier, expert_count + tensor_count - 1)
            for before in range(e):
                swap(before).start()
        elif e > BARRIER_AT:
            swap(e - 1).start()

    swap(local_experts - 1).start()

    @pl.loop(0, local_experts)
    def _(e):
        swap(e).wait_recv()

    home = c // group == z
    spot_here = z * group + lax.rem(c, group)

    def along(source):
        spot = z * group + lax.rem(source, group)
        return remote(
            passing.at[source], result.at[r, spot], z_send.at[source], z_recv.at[spot], (c, source // group, r)
        )

    @pl.when(home)
    def _():
        result[r, c] = mine[placement[c]]

    @pl.when(jnp.logical_not(home))
    def _():
        passing[c] = mine[placement[c]]

    def plane(s):
        return remote(staged.at[s], passing.at[c], plane_send.at[s], plane_recv.at[c], (s, z, r))

    def plane_home(s):
        return remote(staged.at[s], result.at[r, spot_here], plane_send.at[s], z_recv.at[spot_here], (s, z, r))

    def plane_from(source):
        return remote(staged.at[source], passing.at[source], plane_send.at[source], plane_recv.at[source], (source, z, r))

    def shifted(dx, dy):
        return lax.rem(c // side + dx + side, side) * side + lax.rem(lax.rem(c, side) + dy + side, side)

    def group_turns(place):
        which = lax.rem(place + z + 2 * r, len(TURNS))
        steps = []
        for axis in range(2):
            packed = [sum((turn[axis] % side) << (4 * k) for k, turn in enumerate(turns)) for turns in TURNS]
            code = jnp.int32(packed[0])
            for g in range(1, len(TURNS)):
                code = jnp.where(which == g, packed[g], code)
            steps.append([(code >> (4 * k)) & (side - 1) for k in range(WIDTH)])
        return tuple(zip(*steps))

    def issue(turns):
        targets = [shifted(dx, dy) for dx, dy in turns]
        for s in targets:
            staged[s] = mine[placement[s]]
        for s in targets:

            @pl.when((s != c) & home)
            def _():
                plane_home(s).start()

            @pl.when((s != c) & jnp.logical_not(home))
            def _():
                plane(s).start()

    def forward(turns):
        for dx, dy in turns:
            source = shifted(side - dx, side - dy)

            @pl.when((source != c) & (source // group != z))
            def _():
                plane_from(source).wait_recv()
                along(source).start()

    @pl.when(jnp.logical_not(home))
    def _():
        along(c).start()

    order = [group_turns(place) for place in range(len(TURNS))]
    for turns in order[:AHEAD]:
        issue(turns)
    for g, turns in enumerate(order):
        forward(turns)
        if g + AHEAD < len(order):
            issue(order[g + AHEAD])

    @pl.loop(0, local_experts)
    def _(e):
        swap(e).wait_send()

    @pl.loop(0, slots)
    def _(s):
        @pl.when(s != c)
        def _():
            plane(s).wait_send()

    def last(spot):
        return remote(
            result.at[r, spot], result.at[r, spot], last_send.at[spot], last_recv.at[spot], (c, z, 1 - r)
        )

    def arrived(spot):
        return remote(result.at[r, spot], result.at[r, spot], z_send.at[spot], z_recv.at[spot], (c, z, 1 - r))

    def last_from(spot):
        return remote(result.at[1 - r, spot], result.at[1 - r, spot], last_send.at[spot], last_recv.at[spot], (c, z, 1 - r))

    @pl.loop(0, slots)
    def _(step):
        far = (step // group + 1) // 2
        away = jnp.where(lax.rem(step // group, 2) == 1, far, tensor_count - far)
        spot = lax.rem(z + away, tensor_count) * group + lax.rem(step, group)

        @pl.when(jnp.logical_not(home & (spot == c)))
        def _():
            arrived(spot).wait_recv()

        last(spot).start()

    @pl.loop(0, slots)
    def _(s):
        @pl.when(s // group != z)
        def _():
            along(s).wait_send()

        last(s).wait_send()

    @pl.loop(0, slots)
    def _(s):
        last_from(s).wait_recv()


def push(trained, snapshot, changed, placement):
    block_rows, _, local_experts = changed.shape
    slots = placement.shape[0]
    sizes = (lax.axis_size("expert"), lax.axis_size("tensor"), local_experts, block_rows)
    dma = pltpu.SemaphoreType.DMA

    def kernel(a, b, c, d, result, *refs):
        new_bufs, old_bufs, refs = refs[:local_experts], refs[local_experts : 2 * local_experts], refs[2 * local_experts :]
        push_kernel(sizes, a, b, c, d, result, new_bufs, old_bufs, *refs[:7], refs[7:])

    return pl.pallas_call(
        kernel,
        name="push",
        out_shape=pltpu.VMEM((2, slots, ROWS, BLK), jnp.bfloat16),
        in_specs=[
            pl.BlockSpec(memory_space=pltpu.HBM),
            pl.BlockSpec(memory_space=pltpu.HBM),
            pl.BlockSpec(memory_space=pltpu.HBM),
            pl.BlockSpec(memory_space=pltpu.HBM),
        ],
        out_specs=pl.BlockSpec(memory_space=pltpu.VMEM),
        scratch_shapes=[
            *[pltpu.VMEM(trained.shape[1:], jnp.float32) for _ in range(local_experts)],
            *[pltpu.VMEM(snapshot.shape[1:], jnp.bfloat16) for _ in range(local_experts)],
            pltpu.SMEM(changed.shape, jnp.int32),
            pltpu.SMEM(placement.shape, jnp.int32),
            pltpu.VMEM((BLK, 2 * BLK), jnp.bfloat16),
            pltpu.VMEM((slots, ROWS, BLK), jnp.bfloat16),
            pltpu.VMEM((local_experts, ROWS, BLK), jnp.bfloat16),
            pltpu.VMEM((slots, ROWS, BLK), jnp.bfloat16),
            pltpu.VMEM((slots, ROWS, BLK), jnp.bfloat16),
            dma((2, local_experts)),
            dma((2,)),
            dma((local_experts,)),
            dma((local_experts,)),
            dma((slots,)),
            dma((slots,)),
            dma((slots,)),
            dma((slots,)),
            dma((slots,)),
            dma((slots,)),
        ],
        compiler_params=pltpu.CompilerParams(collective_id=0, has_side_effects=True, vmem_limit_bytes=60 * 1024 * 1024),
    )(trained, snapshot, changed, placement)


def spread_kernel(sizes, tiles, out, image, sems):
    tensor_count, group, block_rows = sizes

    def write(z):
        rows = pl.ds(pl.multiple_of(z * block_rows * BLK, BLK), block_rows * BLK)
        return pltpu.make_async_copy(image.at[z], out.at[0, rows, :], sems.at[z])

    @pl.loop(0, tensor_count)
    def _(z):
        for j in range(group):
            index = z * group + j
            spots = []
            for k in range(MOST):
                row = HALF * BLK + (k % HALF) * (META // HALF)
                spots.append(tiles[k // HALF, index, row : row + 1, :])
            chunk = 32
            for b in range(block_rows):
                masks = [jnp.broadcast_to(spots[k] == jnp.bfloat16(b), (chunk, BLK)) for k in range(MOST)]
                for first in range(0, BLK, chunk):
                    value = jnp.zeros((chunk, BLK), jnp.bfloat16)
                    for k in range(MOST):
                        row = (k % HALF) * BLK + first
                        value = jnp.where(masks[k], tiles[k // HALF, index, row : row + chunk, :], value)
                    image[z, b * BLK + first : b * BLK + first + chunk, j * BLK : (j + 1) * BLK] = value
        write(z).start()

    @pl.loop(0, tensor_count)
    def _(z):
        write(z).wait()


def spread(tiles, block_rows):
    tensor_count = lax.axis_size("tensor")
    group = tiles.shape[1] // tensor_count
    rows = block_rows * BLK

    def kernel(tiles_ref, out, image, sems):
        spread_kernel((tensor_count, group, block_rows), tiles_ref, out, image, sems)

    return pl.pallas_call(
        kernel,
        name="spread",
        out_shape=jax.ShapeDtypeStruct((1, tensor_count * rows, group * BLK), jnp.bfloat16),
        in_specs=[pl.BlockSpec(memory_space=pltpu.VMEM)],
        out_specs=pl.BlockSpec(memory_space=pl.ANY),
        scratch_shapes=[
            pltpu.VMEM((tensor_count, rows, group * BLK), jnp.bfloat16),
            pltpu.SemaphoreType.DMA((tensor_count,)),
        ],
        compiler_params=pltpu.CompilerParams(vmem_limit_bytes=24 * 1024 * 1024),
    )(tiles)


def body(trained, snapshot, changed, placement):
    local_experts, local_rows, _ = trained.shape
    block_rows = local_rows // BLK
    blocks = (local_experts, block_rows, BLK, BLK)
    tiles = push(trained.reshape(blocks), snapshot.reshape(blocks), changed.transpose(1, 2, 0), placement)
    return spread(tiles, block_rows)


def solution(mesh):
    in_specs = (
        P("replica", "tensor", "expert"),
        P("replica", "tensor", "expert"),
        P("replica", "tensor", "expert"),
        P(),
    )
    out_specs = P("expert", None, "tensor")
    return jax.shard_map(body, mesh=mesh, in_specs=in_specs, out_specs=out_specs, check_vma=False)
```

```python
import math

import jax
import jax.numpy as jnp
from jax import lax
from jax.experimental import pallas as pl
from jax.experimental.pallas import tpu as pltpu
from jax.sharding import PartitionSpec as P

MESH = pl.DeviceIdType.MESH
BLK = 128
MOST = 4
HALF = MOST // 2
META = 8
ROWS = HALF * BLK + META
BARRIER_AT = 4
WINDOW = 10
RAMP = 10
CHUNK = 64
TOGETHER = 2
PIECES = ((0, BLK), (BLK, ROWS - BLK))
TURNS = (
    ((1, 0), (-1, 0), (0, 1), (0, -1)),
    ((1, 1), (-1, -1), (2, 0), (0, 2)),
    ((1, -1), (-1, 1), (2, 2), (0, 0)),
    ((2, 1), (2, -1), (1, 2), (-1, 2)),
)


def sign_table(rows, cols):
    shared = lax.broadcasted_iota(jnp.int32, (rows, cols), 0) & (
        lax.broadcasted_iota(jnp.int32, (rows, cols), 1) & (BLK - 1)
    )
    shared = shared ^ (shared >> 4)
    shared = shared ^ (shared >> 2)
    shared = shared ^ (shared >> 1)
    return (1 - 2 * (shared & 1)).astype(jnp.float32).astype(jnp.bfloat16)


def push_kernel(
    sizes, trained, snapshot, changed_in, placement_in, result, new_bufs, old_bufs, changed, placement, table, mine, other, staged, passing, sems
):
    expert_count, tensor_count, local_experts, block_rows = sizes
    (in_sem, table_sem, swap_send, swap_recv, plane_send, plane_recv, z_send, z_recv, last_send, last_recv) = sems
    c = lax.axis_index("expert")
    z = lax.axis_index("tensor")
    r = lax.axis_index("replica")
    slots = expert_count
    group = expert_count // tensor_count
    side = math.isqrt(expert_count)

    small_loads = (
        pltpu.make_async_copy(changed_in, changed, table_sem.at[0]),
        pltpu.make_async_copy(placement_in, placement, table_sem.at[1]),
    )
    loads = [
        (
            pltpu.make_async_copy(trained.at[e], new_bufs[e], in_sem.at[0, e]),
            pltpu.make_async_copy(snapshot.at[e], old_bufs[e], in_sem.at[1, e]),
        )
        for e in range(local_experts)
    ]
    for load in small_loads:
        load.start()
    for pair in loads:
        for load in pair:
            load.start()

    barrier = pltpu.get_barrier_semaphore()

    pl.semaphore_signal(barrier, inc=1, device_id=(c, z, 1 - r), device_id_type=MESH)

    @pl.loop(1, expert_count)
    def _(step):
        pl.semaphore_signal(barrier, inc=1, device_id=(lax.rem(c + step, expert_count), z, r), device_id_type=MESH)

    @pl.loop(1, tensor_count)
    def _(step):
        pl.semaphore_signal(barrier, inc=1, device_id=(c, lax.rem(z + step, tensor_count), r), device_id_type=MESH)

    table[...] = sign_table(BLK, 2 * BLK)
    for load in small_loads:
        load.wait()

    def remote(src, dst, send_sem, recv_sem, device):
        return pltpu.make_async_remote_copy(
            src_ref=src, dst_ref=dst, send_sem=send_sem, recv_sem=recv_sem, device_id=device, device_id_type=MESH
        )

    def swap(e):
        return remote(other.at[e], mine.at[r * local_experts + e], swap_send, swap_recv, (c, z, 1 - r))

    row_ids = lax.broadcasted_iota(jnp.int32, (META, BLK), 0)

    def chosen(e):
        count = jnp.int32(0)
        spots = [jnp.int32(block_rows)] * MOST
        picks = [jnp.int32(0)] * MOST
        for b in range(block_rows):
            flag = changed[b, 0, e]
            for k in range(MOST):
                hit = (flag == 1) & (count == k)
                spots[k] = jnp.where(hit, b, spots[k])
                picks[k] = jnp.where(hit, b, picks[k])
            count = count + flag
        return spots, picks

    for start in range(0, local_experts, TOGETHER):
        batch = range(start, start + TOGETHER)
        places = [chosen(e) for e in batch]
        for e in batch:
            for load in loads[e]:
                load.wait()
        highs, lows = [], []
        for e, (_, picks) in zip(batch, places):
            for pick in picks:
                delta = new_bufs[e][pick] - old_bufs[e][pick].astype(jnp.float32)
                high = delta.astype(jnp.bfloat16)
                highs.append(high)
                lows.append((delta - high.astype(jnp.float32)).astype(jnp.bfloat16))
        parts = jnp.concatenate([jnp.concatenate(highs, axis=1), jnp.concatenate(lows, axis=1)], axis=0)
        coded = jnp.dot(table[...], parts, preferred_element_type=jnp.float32) * (1.0 / math.sqrt(BLK))
        coded = coded.astype(jnp.bfloat16)

        def store(ref, index, i, first, coded=coded, places=places):
            for k in range(HALF):
                column = (i * MOST + first + k) * BLK
                ref[index, k * BLK : (k + 1) * BLK, :] = coded[:, column : column + BLK]
            spots = places[i][0]
            spot = jnp.where(row_ids < META // 2, spots[first], spots[first + 1])
            ref[index, HALF * BLK : ROWS, :] = spot.astype(jnp.float32).astype(jnp.bfloat16)

        for low in range(2):

            @pl.when(r == low)
            def _(low=low):
                for i, e in enumerate(batch):
                    store(mine, r * local_experts + e, i, low * HALF)
                    store(other, e, i, (1 - low) * HALF)

        if start == BARRIER_AT:
            pl.semaphore_wait(barrier, expert_count + tensor_count - 1)
            for e in range(start):
                swap(e).start()
        elif start > BARRIER_AT:
            for e in range(start - TOGETHER, start):
                swap(e).start()

    for e in range(local_experts - TOGETHER, local_experts):
        swap(e).start()

    arrivals = mine.at[pl.ds((1 - r) * local_experts, local_experts)]
    pltpu.make_async_copy(arrivals, arrivals, swap_recv).wait()

    home = c // group == z
    spot_here = z * group + lax.rem(c, group)

    def along(source, piece):
        spot = z * group + lax.rem(source, group)
        rows = pl.ds(*PIECES[piece])
        return remote(
            passing.at[source, rows], result.at[r, spot, rows], z_send, z_recv.at[spot], (c, source // group, r)
        )

    @pl.when(home)
    def _():
        result[r, c] = mine[placement[c]]

    @pl.when(jnp.logical_not(home))
    def _():
        passing[c] = mine[placement[c]]

    def plane(s, piece):
        rows = pl.ds(*PIECES[piece])
        return remote(staged.at[s, rows], passing.at[c, rows], plane_send, plane_recv.at[piece, c], (s, z, r))

    def plane_home(s, piece):
        rows = pl.ds(*PIECES[piece])
        return remote(staged.at[s, rows], result.at[r, spot_here, rows], plane_send, z_recv.at[spot_here], (s, z, r))

    def plane_from(source, piece):
        rows = pl.ds(*PIECES[piece])
        return remote(
            staged.at[source, rows], passing.at[source, rows], plane_send, plane_recv.at[piece, source], (source, z, r)
        )

    def shifted(dx, dy):
        return lax.rem(c // side + dx + side, side) * side + lax.rem(lax.rem(c, side) + dy + side, side)

    def group_turns(place):
        which = lax.rem(place + z + 2 * r, len(TURNS))
        steps = []
        for axis in range(2):
            packed = [sum((turn[axis] % side) << (4 * k) for k, turn in enumerate(turns)) for turns in TURNS]
            code = jnp.int32(packed[0])
            for g in range(1, len(TURNS)):
                code = jnp.where(which == g, packed[g], code)
            steps.append([(code >> (4 * k)) & (side - 1) for k in range(len(TURNS[0]))])
        return list(zip(*steps))

    def stage(turn):
        s = shifted(*turn)
        staged[s] = mine[placement[s]]

    def issue(turn, piece):
        s = shifted(*turn)

        @pl.when((s != c) & home)
        def _():
            plane_home(s, piece).start()

        @pl.when((s != c) & jnp.logical_not(home))
        def _():
            plane(s, piece).start()

    def forward(turn, piece):
        source = shifted(side - turn[0], side - turn[1])

        @pl.when((source != c) & (source // group != z))
        def _():
            plane_from(source, piece).wait_recv()
            along(source, piece).start()

    order = sum([group_turns(place) for place in range(len(TURNS))], [])
    pieces = [(turn, piece) for turn in order for piece in range(len(PIECES))]
    early = -(-RAMP // len(PIECES))
    for turn in order[:early]:
        stage(turn)
    for item in pieces[:RAMP]:
        issue(*item)

    @pl.when(jnp.logical_not(home))
    def _():
        for piece in range(len(PIECES)):
            along(c, piece).start()

    for turn in order[early:]:
        stage(turn)
    issued = RAMP
    for i, item in enumerate(pieces):
        forward(*item)
        upto = min(i + 1 + min(RAMP + i + 1, WINDOW), len(pieces))
        for later in pieces[issued:upto]:
            issue(*later)
        issued = max(issued, upto)

    def settle(ref, sem):
        pltpu.make_async_copy(ref, ref, sem).wait()

    settle(other, swap_send)
    settle(staged.at[pl.ds(0, slots - 1)], plane_send)

    def last(spot):
        return remote(
            result.at[r, spot], result.at[r, spot], last_send, last_recv, (c, z, 1 - r)
        )

    def arrived(spot):
        return remote(result.at[r, spot], result.at[r, spot], z_send, z_recv.at[spot], (c, z, 1 - r))

    @pl.loop(0, slots)
    def _(step):
        far = (step // group + 1) // 2
        away = jnp.where(lax.rem(step // group, 2) == 1, far, tensor_count - far)
        spot = lax.rem(z + away, tensor_count) * group + lax.rem(step, group)

        @pl.when(jnp.logical_not(home & (spot == c)))
        def _():
            arrived(spot).wait_recv()

        last(spot).start()

    settle(passing.at[pl.ds(0, slots - group)], z_send)
    settle(result.at[r], last_send)
    settle(result.at[1 - r], last_recv)


def push(trained, snapshot, changed, placement):
    block_rows, _, local_experts = changed.shape
    slots = placement.shape[0]
    sizes = (lax.axis_size("expert"), lax.axis_size("tensor"), local_experts, block_rows)
    dma = pltpu.SemaphoreType.DMA

    def kernel(a, b, c, d, result, *refs):
        new_bufs, old_bufs, refs = refs[:local_experts], refs[local_experts : 2 * local_experts], refs[2 * local_experts :]
        push_kernel(sizes, a, b, c, d, result, new_bufs, old_bufs, *refs[:7], refs[7:])

    return pl.pallas_call(
        kernel,
        name="push",
        out_shape=pltpu.VMEM((2, slots, ROWS, BLK), jnp.bfloat16),
        in_specs=[
            pl.BlockSpec(memory_space=pltpu.HBM),
            pl.BlockSpec(memory_space=pltpu.HBM),
            pl.BlockSpec(memory_space=pltpu.HBM),
            pl.BlockSpec(memory_space=pltpu.HBM),
        ],
        out_specs=pl.BlockSpec(memory_space=pltpu.VMEM),
        scratch_shapes=[
            *[pltpu.VMEM(trained.shape[1:], jnp.float32) for _ in range(local_experts)],
            *[pltpu.VMEM(snapshot.shape[1:], jnp.bfloat16) for _ in range(local_experts)],
            pltpu.SMEM(changed.shape, jnp.int32),
            pltpu.SMEM(placement.shape, jnp.int32),
            pltpu.VMEM((BLK, 2 * BLK), jnp.bfloat16),
            pltpu.VMEM((slots, ROWS, BLK), jnp.bfloat16),
            pltpu.VMEM((local_experts, ROWS, BLK), jnp.bfloat16),
            pltpu.VMEM((slots, ROWS, BLK), jnp.bfloat16),
            pltpu.VMEM((slots, ROWS, BLK), jnp.bfloat16),
            dma((2, local_experts)),
            dma((2,)),
            dma,
            dma,
            dma,
            dma((len(PIECES), slots)),
            dma,
            dma((slots,)),
            dma,
            dma,
        ],
        compiler_params=pltpu.CompilerParams(collective_id=0, has_side_effects=True, vmem_limit_bytes=60 * 1024 * 1024),
    )(trained, snapshot, changed, placement)


def spread_kernel(sizes, tiles, out, image, sems):
    tensor_count, group, block_rows = sizes

    def write(z):
        rows = pl.ds(pl.multiple_of(z * block_rows * BLK, BLK), block_rows * BLK)
        return pltpu.make_async_copy(image.at[z], out.at[0, rows, :], sems.at[z])

    @pl.loop(0, tensor_count)
    def _(z):
        for j in range(group):
            index = z * group + j
            spots = []
            for k in range(MOST):
                row = HALF * BLK + (k % HALF) * (META // HALF)
                spots.append(jnp.broadcast_to(tiles[k // HALF, index, row : row + 1, :], (CHUNK, BLK)))
            for first in range(0, BLK, CHUNK):
                values = []
                for k in range(MOST):
                    row = (k % HALF) * BLK + first
                    values.append(tiles[k // HALF, index, row : row + CHUNK, :])
                for b in range(block_rows):
                    value = jnp.zeros((CHUNK, BLK), jnp.bfloat16)
                    for k in range(MOST):
                        value = jnp.where(spots[k] == jnp.bfloat16(b), values[k], value)
                    image[z, b * BLK + first : b * BLK + first + CHUNK, j * BLK : (j + 1) * BLK] = value
        write(z).start()

    @pl.loop(0, tensor_count)
    def _(z):
        write(z).wait()


def spread(tiles, block_rows):
    tensor_count = lax.axis_size("tensor")
    group = tiles.shape[1] // tensor_count
    rows = block_rows * BLK

    def kernel(tiles_ref, out, image, sems):
        spread_kernel((tensor_count, group, block_rows), tiles_ref, out, image, sems)

    return pl.pallas_call(
        kernel,
        name="spread",
        out_shape=jax.ShapeDtypeStruct((1, tensor_count * rows, group * BLK), jnp.bfloat16),
        in_specs=[pl.BlockSpec(memory_space=pltpu.VMEM)],
        out_specs=pl.BlockSpec(memory_space=pl.ANY),
        scratch_shapes=[
            pltpu.VMEM((tensor_count, rows, group * BLK), jnp.bfloat16),
            pltpu.SemaphoreType.DMA((tensor_count,)),
        ],
        compiler_params=pltpu.CompilerParams(vmem_limit_bytes=24 * 1024 * 1024),
    )(tiles)


def body(trained, snapshot, changed, placement):
    local_experts, local_rows, _ = trained.shape
    block_rows = local_rows // BLK
    blocks = (local_experts, block_rows, BLK, BLK)
    tiles = push(trained.reshape(blocks), snapshot.reshape(blocks), changed.transpose(1, 2, 0), placement)
    return spread(tiles, block_rows)


def solution(mesh):
    in_specs = (
        P("replica", "tensor", "expert"),
        P("replica", "tensor", "expert"),
        P("replica", "tensor", "expert"),
        P(),
    )
    out_specs = P("expert", None, "tensor")
    return jax.shard_map(body, mesh=mesh, in_specs=in_specs, out_specs=out_specs, check_vma=False)
```

```python
import math

import jax
import jax.numpy as jnp
from jax import lax
from jax.experimental import pallas as pl
from jax.experimental.pallas import tpu as pltpu
from jax.sharding import PartitionSpec as P

MESH = pl.DeviceIdType.MESH
BLK = 128
MOST = 4
HALF = MOST // 2
META = 8
ROWS = HALF * BLK + META
BARRIER_AT = 4
WINDOW = 10
RAMP = 10
CHUNK = 64
TOGETHER = 2
PIECES = ((0, BLK), (BLK, ROWS - BLK))
TURNS = (
    ((0, 1), (0, -1), (1, 0), (-1, 0)),
    ((2, 0), (0, 2), (1, 1), (-1, -1)),
    ((1, -1), (-1, 1), (2, 2), (0, 0)),
    ((2, 1), (2, -1), (1, 2), (-1, 2)),
)


def sign_table(rows, cols):
    shared = lax.broadcasted_iota(jnp.int32, (rows, cols), 0) & (
        lax.broadcasted_iota(jnp.int32, (rows, cols), 1) & (BLK - 1)
    )
    shared = shared ^ (shared >> 4)
    shared = shared ^ (shared >> 2)
    shared = shared ^ (shared >> 1)
    return (1 - 2 * (shared & 1)).astype(jnp.float32).astype(jnp.bfloat16)


def push_kernel(
    sizes, trained, snapshot, changed_in, placement_in, result, new_bufs, old_bufs, changed, placement, table, mine, other, staged, passing, sems
):
    expert_count, tensor_count, local_experts, block_rows = sizes
    (in_sem, table_sem, swap_send, swap_recv, plane_send, plane_recv, z_send, z_recv, last_send, last_recv) = sems
    c = lax.axis_index("expert")
    z = lax.axis_index("tensor")
    r = lax.axis_index("replica")
    slots = expert_count
    group = expert_count // tensor_count
    side = math.isqrt(expert_count)

    small_loads = (
        pltpu.make_async_copy(changed_in, changed, table_sem.at[0]),
        pltpu.make_async_copy(placement_in, placement, table_sem.at[1]),
    )
    loads = [
        (
            pltpu.make_async_copy(trained.at[e], new_bufs[e], in_sem.at[0, e]),
            pltpu.make_async_copy(snapshot.at[e], old_bufs[e], in_sem.at[1, e]),
        )
        for e in range(local_experts)
    ]
    for load in (*small_loads, *loads[0]):
        load.start()

    barrier = pltpu.get_barrier_semaphore()
    for step in range(1, tensor_count):
        pl.semaphore_signal(barrier, inc=1, device_id=(c, lax.rem(z + step, tensor_count), r), device_id_type=MESH)
    for step in range(1, expert_count):
        pl.semaphore_signal(barrier, inc=1, device_id=(lax.rem(c + step, expert_count), z, r), device_id_type=MESH)
    pl.semaphore_signal(barrier, inc=1, device_id=(c, z, 1 - r), device_id_type=MESH)

    for pair in loads[1:]:
        for load in pair:
            load.start()

    table[...] = sign_table(BLK, 2 * BLK)
    for load in small_loads:
        load.wait()

    def remote(src, dst, send_sem, recv_sem, device):
        return pltpu.make_async_remote_copy(
            src_ref=src, dst_ref=dst, send_sem=send_sem, recv_sem=recv_sem, device_id=device, device_id_type=MESH
        )

    def swap(e):
        return remote(other.at[e], mine.at[r * local_experts + e], swap_send, swap_recv, (c, z, 1 - r))

    row_ids = lax.broadcasted_iota(jnp.int32, (META, BLK), 0)

    def chosen(e):
        count = jnp.int32(0)
        spots = [jnp.int32(block_rows)] * MOST
        picks = [jnp.int32(0)] * MOST
        for b in range(block_rows):
            flag = changed[b, 0, e]
            for k in range(MOST):
                hit = (flag == 1) & (count == k)
                spots[k] = jnp.where(hit, b, spots[k])
                picks[k] = jnp.where(hit, b, picks[k])
            count = count + flag
        return spots, picks

    for start in range(0, local_experts, TOGETHER):
        batch = range(start, start + TOGETHER)
        places = [chosen(e) for e in batch]
        for e in batch:
            for load in loads[e]:
                load.wait()
        highs, lows = [], []
        for e, (_, picks) in zip(batch, places):
            for pick in picks:
                delta = new_bufs[e][pick] - old_bufs[e][pick].astype(jnp.float32)
                high = delta.astype(jnp.bfloat16)
                highs.append(high)
                lows.append((delta - high.astype(jnp.float32)).astype(jnp.bfloat16))
        parts = jnp.concatenate([jnp.concatenate(highs, axis=1), jnp.concatenate(lows, axis=1)], axis=0)
        coded = jnp.dot(table[...], parts, preferred_element_type=jnp.float32) * (1.0 / math.sqrt(BLK))
        coded = coded.astype(jnp.bfloat16)

        def store(ref, index, i, first, coded=coded, places=places):
            for k in range(HALF):
                column = (i * MOST + first + k) * BLK
                ref[index, k * BLK : (k + 1) * BLK, :] = coded[:, column : column + BLK]
            spots = places[i][0]
            spot = jnp.where(row_ids < META // 2, spots[first], spots[first + 1])
            ref[index, HALF * BLK : ROWS, :] = spot.astype(jnp.float32).astype(jnp.bfloat16)

        for low in range(2):

            @pl.when(r == low)
            def _(low=low):
                for i, e in enumerate(batch):
                    store(mine, r * local_experts + e, i, low * HALF)
                    store(other, e, i, (1 - low) * HALF)

        if start == BARRIER_AT:
            pl.semaphore_wait(barrier, expert_count + tensor_count - 1)
            for e in range(start):
                swap(e).start()
        elif start > BARRIER_AT:
            for e in range(start - TOGETHER, start):
                swap(e).start()

    for e in range(local_experts - TOGETHER, local_experts):
        swap(e).start()

    arrivals = mine.at[pl.ds((1 - r) * local_experts, local_experts)]
    pltpu.make_async_copy(arrivals, arrivals, swap_recv).wait()

    home = c // group == z
    spot_here = z * group + lax.rem(c, group)

    def along(source, piece):
        spot = z * group + lax.rem(source, group)
        rows = pl.ds(*PIECES[piece])
        return remote(
            passing.at[source, rows], result.at[r, spot, rows], z_send, z_recv.at[spot], (c, source // group, r)
        )

    @pl.when(home)
    def _():
        result[r, c] = mine[placement[c]]

    @pl.when(jnp.logical_not(home))
    def _():
        passing[c] = mine[placement[c]]

    def plane(s, piece):
        rows = pl.ds(*PIECES[piece])
        return remote(staged.at[s, rows], passing.at[c, rows], plane_send, plane_recv.at[piece, c], (s, z, r))

    def plane_home(s, piece):
        rows = pl.ds(*PIECES[piece])
        return remote(staged.at[s, rows], result.at[r, spot_here, rows], plane_send, z_recv.at[spot_here], (s, z, r))

    def plane_from(source, piece):
        rows = pl.ds(*PIECES[piece])
        return remote(
            staged.at[source, rows], passing.at[source, rows], plane_send, plane_recv.at[piece, source], (source, z, r)
        )

    def shifted(dx, dy):
        return lax.rem(c // side + dx + side, side) * side + lax.rem(lax.rem(c, side) + dy + side, side)

    def group_turns(place):
        which = lax.rem(place + z + 2 * r, len(TURNS))
        steps = []
        for axis in range(2):
            packed = [sum((turn[axis] % side) << (4 * k) for k, turn in enumerate(turns)) for turns in TURNS]
            code = jnp.int32(packed[0])
            for g in range(1, len(TURNS)):
                code = jnp.where(which == g, packed[g], code)
            steps.append([(code >> (4 * k)) & (side - 1) for k in range(len(TURNS[0]))])
        return list(zip(*steps))

    def stage(turn):
        s = shifted(*turn)
        staged[s] = mine[placement[s]]

    def issue(turn, piece):
        s = shifted(*turn)

        @pl.when((s != c) & home)
        def _():
            plane_home(s, piece).start()

        @pl.when((s != c) & jnp.logical_not(home))
        def _():
            plane(s, piece).start()

    def forward(turn, piece):
        source = shifted(side - turn[0], side - turn[1])

        @pl.when((source != c) & (source // group != z))
        def _():
            plane_from(source, piece).wait_recv()
            along(source, piece).start()

    order = sum([group_turns(place) for place in range(len(TURNS))], [])
    pieces = [(turn, piece) for turn in order for piece in range(len(PIECES))]
    early = -(-RAMP // len(PIECES))
    for turn in order[:early]:
        stage(turn)
    for item in pieces[:RAMP]:
        issue(*item)

    @pl.when(jnp.logical_not(home))
    def _():
        for piece in range(len(PIECES)):
            along(c, piece).start()

    for turn in order[early:]:
        stage(turn)
    issued = RAMP
    for i, item in enumerate(pieces):
        forward(*item)
        upto = min(i + 1 + min(RAMP + i + 1, WINDOW), len(pieces))
        for later in pieces[issued:upto]:
            issue(*later)
        issued = max(issued, upto)

    def settle(ref, sem):
        pltpu.make_async_copy(ref, ref, sem).wait()

    settle(other, swap_send)
    settle(staged.at[pl.ds(0, slots - 1)], plane_send)

    def last(spot):
        return remote(
            result.at[r, spot], result.at[r, spot], last_send, last_recv, (c, z, 1 - r)
        )

    def arrived(spot):
        return remote(result.at[r, spot], result.at[r, spot], z_send, z_recv.at[spot], (c, z, 1 - r))

    @pl.loop(0, slots)
    def _(step):
        far = (step // group + 1) // 2
        away = jnp.where(lax.rem(step // group, 2) == 1, far, tensor_count - far)
        spot = lax.rem(z + away, tensor_count) * group + lax.rem(step, group)

        @pl.when(jnp.logical_not(home & (spot == c)))
        def _():
            arrived(spot).wait_recv()

        last(spot).start()

    settle(passing.at[pl.ds(0, slots - group)], z_send)
    settle(result.at[r], last_send)
    settle(result.at[1 - r], last_recv)


def push(trained, snapshot, changed, placement):
    block_rows, _, local_experts = changed.shape
    slots = placement.shape[0]
    sizes = (lax.axis_size("expert"), lax.axis_size("tensor"), local_experts, block_rows)
    dma = pltpu.SemaphoreType.DMA

    def kernel(a, b, c, d, result, *refs):
        new_bufs, old_bufs, refs = refs[:local_experts], refs[local_experts : 2 * local_experts], refs[2 * local_experts :]
        push_kernel(sizes, a, b, c, d, result, new_bufs, old_bufs, *refs[:7], refs[7:])

    return pl.pallas_call(
        kernel,
        name="push",
        out_shape=pltpu.VMEM((2, slots, ROWS, BLK), jnp.bfloat16),
        in_specs=[
            pl.BlockSpec(memory_space=pltpu.HBM),
            pl.BlockSpec(memory_space=pltpu.HBM),
            pl.BlockSpec(memory_space=pltpu.HBM),
            pl.BlockSpec(memory_space=pltpu.HBM),
        ],
        out_specs=pl.BlockSpec(memory_space=pltpu.VMEM),
        scratch_shapes=[
            *[pltpu.VMEM(trained.shape[1:], jnp.float32) for _ in range(local_experts)],
            *[pltpu.VMEM(snapshot.shape[1:], jnp.bfloat16) for _ in range(local_experts)],
            pltpu.SMEM(changed.shape, jnp.int32),
            pltpu.SMEM(placement.shape, jnp.int32),
            pltpu.VMEM((BLK, 2 * BLK), jnp.bfloat16),
            pltpu.VMEM((slots, ROWS, BLK), jnp.bfloat16),
            pltpu.VMEM((local_experts, ROWS, BLK), jnp.bfloat16),
            pltpu.VMEM((slots, ROWS, BLK), jnp.bfloat16),
            pltpu.VMEM((slots, ROWS, BLK), jnp.bfloat16),
            dma((2, local_experts)),
            dma((2,)),
            dma,
            dma,
            dma,
            dma((len(PIECES), slots)),
            dma,
            dma((slots,)),
            dma,
            dma,
        ],
        compiler_params=pltpu.CompilerParams(collective_id=0, has_side_effects=True, vmem_limit_bytes=60 * 1024 * 1024),
    )(trained, snapshot, changed, placement)


def spread_kernel(sizes, tiles, out, image, sems):
    tensor_count, group, block_rows = sizes

    def write(z):
        rows = pl.ds(pl.multiple_of(z * block_rows * BLK, BLK), block_rows * BLK)
        return pltpu.make_async_copy(image.at[z], out.at[0, rows, :], sems.at[z])

    @pl.loop(0, tensor_count)
    def _(z):
        for j in range(group):
            index = z * group + j
            spots = []
            for k in range(MOST):
                row = HALF * BLK + (k % HALF) * (META // HALF)
                spots.append(jnp.broadcast_to(tiles[k // HALF, index, row : row + 1, :], (CHUNK, BLK)))
            for first in range(0, BLK, CHUNK):
                values = []
                for k in range(MOST):
                    row = (k % HALF) * BLK + first
                    values.append(tiles[k // HALF, index, row : row + CHUNK, :])
                for b in range(block_rows):
                    value = jnp.zeros((CHUNK, BLK), jnp.bfloat16)
                    for k in range(MOST):
                        value = jnp.where(spots[k] == jnp.bfloat16(b), values[k], value)
                    image[z, b * BLK + first : b * BLK + first + CHUNK, j * BLK : (j + 1) * BLK] = value
        write(z).start()

    @pl.loop(0, tensor_count)
    def _(z):
        write(z).wait()


def spread(tiles, block_rows):
    tensor_count = lax.axis_size("tensor")
    group = tiles.shape[1] // tensor_count
    rows = block_rows * BLK

    def kernel(tiles_ref, out, image, sems):
        spread_kernel((tensor_count, group, block_rows), tiles_ref, out, image, sems)

    return pl.pallas_call(
        kernel,
        name="spread",
        out_shape=jax.ShapeDtypeStruct((1, tensor_count * rows, group * BLK), jnp.bfloat16),
        in_specs=[pl.BlockSpec(memory_space=pltpu.VMEM)],
        out_specs=pl.BlockSpec(memory_space=pl.ANY),
        scratch_shapes=[
            pltpu.VMEM((tensor_count, rows, group * BLK), jnp.bfloat16),
            pltpu.SemaphoreType.DMA((tensor_count,)),
        ],
        compiler_params=pltpu.CompilerParams(vmem_limit_bytes=24 * 1024 * 1024),
    )(tiles)


def body(trained, snapshot, changed, placement):
    local_experts, local_rows, _ = trained.shape
    block_rows = local_rows // BLK
    blocks = (local_experts, block_rows, BLK, BLK)
    tiles = push(trained.reshape(blocks), snapshot.reshape(blocks), changed.transpose(1, 2, 0), placement)
    return spread(tiles, block_rows)


def solution(mesh):
    in_specs = (
        P("replica", "tensor", "expert"),
        P("replica", "tensor", "expert"),
        P("replica", "tensor", "expert"),
        P(),
    )
    out_specs = P("expert", None, "tensor")
    return jax.shard_map(body, mesh=mesh, in_specs=in_specs, out_specs=out_specs, check_vma=False)
```

```python
import math

import jax
import jax.numpy as jnp
from jax import lax
from jax.experimental import pallas as pl
from jax.experimental.pallas import tpu as pltpu
from jax.sharding import PartitionSpec as P

MESH = pl.DeviceIdType.MESH
BLK = 128
MOST = 4
HALF = MOST // 2
META = 8
ROWS = HALF * BLK + META
BARRIER_AT = 4
WINDOW = 10
RAMP = 10
CHUNK = 64
TOGETHER = 2
PIECES = ((0, BLK), (BLK, ROWS - BLK))
TURNS = (
    ((0, 1), (0, -1), (1, 0), (-1, 0)),
    ((2, 0), (0, 2), (1, 1), (-1, -1)),
    ((1, -1), (-1, 1), (2, 2), (0, 0)),
    ((2, 1), (2, -1), (1, 2), (-1, 2)),
)


def sign_table(rows, cols):
    shared = lax.broadcasted_iota(jnp.int32, (rows, cols), 0) & (
        lax.broadcasted_iota(jnp.int32, (rows, cols), 1) & (BLK - 1)
    )
    shared = shared ^ (shared >> 4)
    shared = shared ^ (shared >> 2)
    shared = shared ^ (shared >> 1)
    return (1 - 2 * (shared & 1)).astype(jnp.float32).astype(jnp.bfloat16)


def push_kernel(
    sizes, trained, snapshot, changed_in, placement_in, result, new_bufs, old_bufs, changed, placement, table, mine, other, staged, passing, sems
):
    expert_count, tensor_count, local_experts, block_rows = sizes
    (in_sem, table_sem, swap_send, swap_recv, plane_send, plane_recv, z_send, z_recv, last_send, last_recv) = sems
    c = lax.axis_index("expert")
    z = lax.axis_index("tensor")
    r = lax.axis_index("replica")
    slots = expert_count
    group = expert_count // tensor_count
    side = math.isqrt(expert_count)

    small_loads = (
        pltpu.make_async_copy(changed_in, changed, table_sem.at[0]),
        pltpu.make_async_copy(placement_in, placement, table_sem.at[1]),
    )
    loads = [
        (
            pltpu.make_async_copy(trained.at[e], new_bufs[e], in_sem.at[0, e]),
            pltpu.make_async_copy(snapshot.at[e], old_bufs[e], in_sem.at[1, e]),
        )
        for e in range(local_experts)
    ]
    for load in (*small_loads, *loads[0]):
        load.start()

    barrier = pltpu.get_barrier_semaphore()
    for step in range(1, tensor_count):
        pl.semaphore_signal(barrier, inc=1, device_id=(c, lax.rem(z + step, tensor_count), r), device_id_type=MESH)
    for step in range(1, expert_count):
        pl.semaphore_signal(barrier, inc=1, device_id=(lax.rem(c + step, expert_count), z, r), device_id_type=MESH)
    pl.semaphore_signal(barrier, inc=1, device_id=(c, z, 1 - r), device_id_type=MESH)

    for pair in loads[1:]:
        for load in pair:
            load.start()

    table[...] = sign_table(BLK, 2 * BLK)
    for load in small_loads:
        load.wait()

    def remote(src, dst, send_sem, recv_sem, device):
        return pltpu.make_async_remote_copy(
            src_ref=src, dst_ref=dst, send_sem=send_sem, recv_sem=recv_sem, device_id=device, device_id_type=MESH
        )

    def swap(e):
        return remote(other.at[e], mine.at[r * local_experts + e], swap_send, swap_recv, (c, z, 1 - r))

    row_ids = lax.broadcasted_iota(jnp.int32, (META, BLK), 0)

    def chosen(e):
        count = jnp.int32(0)
        spots = [jnp.int32(block_rows)] * MOST
        picks = [jnp.int32(0)] * MOST
        for b in range(block_rows):
            flag = changed[b, 0, e]
            for k in range(MOST):
                hit = (flag == 1) & (count == k)
                spots[k] = jnp.where(hit, b, spots[k])
                picks[k] = jnp.where(hit, b, picks[k])
            count = count + flag
        return spots, picks

    for start in range(0, local_experts, TOGETHER):
        batch = range(start, start + TOGETHER)
        places = [chosen(e) for e in batch]
        for e in batch:
            for load in loads[e]:
                load.wait()
        highs, lows = [], []
        for e, (_, picks) in zip(batch, places):
            for pick in picks:
                delta = new_bufs[e][pick] - old_bufs[e][pick].astype(jnp.float32)
                high = delta.astype(jnp.bfloat16)
                highs.append(high)
                lows.append((delta - high.astype(jnp.float32)).astype(jnp.bfloat16))
        parts = jnp.concatenate([jnp.concatenate(highs, axis=1), jnp.concatenate(lows, axis=1)], axis=0)
        coded = jnp.dot(table[...], parts, preferred_element_type=jnp.float32) * (1.0 / math.sqrt(BLK))
        coded = coded.astype(jnp.bfloat16)

        def store(ref, index, i, first, coded=coded, places=places):
            for k in range(HALF):
                column = (i * MOST + first + k) * BLK
                ref[index, k * BLK : (k + 1) * BLK, :] = coded[:, column : column + BLK]
            spots = places[i][0]
            spot = jnp.where(row_ids < META // 2, spots[first], spots[first + 1])
            ref[index, HALF * BLK : ROWS, :] = spot.astype(jnp.float32).astype(jnp.bfloat16)

        for low in range(2):

            @pl.when(r == low)
            def _(low=low):
                for i, e in enumerate(batch):
                    store(mine, r * local_experts + e, i, low * HALF)
                    store(other, e, i, (1 - low) * HALF)

        if start == BARRIER_AT:
            pl.semaphore_wait(barrier, expert_count + tensor_count - 1)
            for e in range(start):
                swap(e).start()
        elif start > BARRIER_AT:
            for e in range(start - TOGETHER, start):
                swap(e).start()

    for e in range(local_experts - TOGETHER, local_experts):
        swap(e).start()

    arrivals = mine.at[pl.ds((1 - r) * local_experts, local_experts)]
    pltpu.make_async_copy(arrivals, arrivals, swap_recv).wait()

    home = c // group == z
    spot_here = z * group + lax.rem(c, group)

    def along(source, piece):
        spot = z * group + lax.rem(source, group)
        rows = pl.ds(*PIECES[piece])
        return remote(
            passing.at[source, rows], result.at[r, spot, rows], z_send, z_recv.at[spot], (c, source // group, r)
        )

    @pl.when(home)
    def _():
        result[r, c] = mine[placement[c]]

    @pl.when(jnp.logical_not(home))
    def _():
        passing[c] = mine[placement[c]]

    def plane(s, piece):
        rows = pl.ds(*PIECES[piece])
        return remote(staged.at[s, rows], passing.at[c, rows], plane_send, plane_recv.at[piece, c], (s, z, r))

    def plane_home(s, piece):
        rows = pl.ds(*PIECES[piece])
        return remote(staged.at[s, rows], result.at[r, spot_here, rows], plane_send, z_recv.at[spot_here], (s, z, r))

    def plane_from(source, piece):
        rows = pl.ds(*PIECES[piece])
        return remote(
            staged.at[source, rows], passing.at[source, rows], plane_send, plane_recv.at[piece, source], (source, z, r)
        )

    def shifted(dx, dy):
        return lax.rem(c // side + dx + side, side) * side + lax.rem(lax.rem(c, side) + dy + side, side)

    def group_turns(place):
        which = lax.rem(place + z + 2 * r, len(TURNS))
        steps = []
        for axis in range(2):
            packed = [sum((turn[axis] % side) << (4 * k) for k, turn in enumerate(turns)) for turns in TURNS]
            code = jnp.int32(packed[0])
            for g in range(1, len(TURNS)):
                code = jnp.where(which == g, packed[g], code)
            steps.append([(code >> (4 * k)) & (side - 1) for k in range(len(TURNS[0]))])
        return list(zip(*steps))

    def stage(turn):
        s = shifted(*turn)
        staged[s] = mine[placement[s]]

    def issue(turn, piece):
        s = shifted(*turn)

        @pl.when((s != c) & home)
        def _():
            plane_home(s, piece).start()

        @pl.when((s != c) & jnp.logical_not(home))
        def _():
            plane(s, piece).start()

    def forward(turn, piece):
        source = shifted(side - turn[0], side - turn[1])

        @pl.when((source != c) & (source // group != z))
        def _():
            plane_from(source, piece).wait_recv()
            along(source, piece).start()

    order = sum([group_turns(place) for place in range(len(TURNS))], [])
    @pl.when(jnp.logical_not(home))
    def _():
        for piece in range(len(PIECES)):
            along(c, piece).start()

    pieces = [(turn, piece) for turn in order for piece in range(len(PIECES))]
    early = -(-RAMP // len(PIECES))
    for turn in order[:early]:
        stage(turn)
    for item in pieces[:RAMP]:
        issue(*item)

    for turn in order[early:]:
        stage(turn)
    issued = RAMP
    for i, item in enumerate(pieces):
        forward(*item)
        upto = min(i + 1 + min(RAMP + i + 1, WINDOW), len(pieces))
        for later in pieces[issued:upto]:
            issue(*later)
        issued = max(issued, upto)

    def settle(ref, sem):
        pltpu.make_async_copy(ref, ref, sem).wait()

    settle(other, swap_send)
    settle(staged.at[pl.ds(0, slots - 1)], plane_send)

    def last(spot):
        return remote(
            result.at[r, spot], result.at[r, spot], last_send, last_recv, (c, z, 1 - r)
        )

    def arrived(spot):
        return remote(result.at[r, spot], result.at[r, spot], z_send, z_recv.at[spot], (c, z, 1 - r))

    @pl.loop(0, slots)
    def _(step):
        far = (step // group + 1) // 2
        away = jnp.where(lax.rem(step // group, 2) == 1, far, tensor_count - far)
        spot = lax.rem(z + away, tensor_count) * group + lax.rem(step, group)

        @pl.when(jnp.logical_not(home & (spot == c)))
        def _():
            arrived(spot).wait_recv()

        last(spot).start()

    settle(passing.at[pl.ds(0, slots - group)], z_send)
    settle(result.at[r], last_send)
    settle(result.at[1 - r], last_recv)


def push(trained, snapshot, changed, placement):
    block_rows, _, local_experts = changed.shape
    slots = placement.shape[0]
    sizes = (lax.axis_size("expert"), lax.axis_size("tensor"), local_experts, block_rows)
    dma = pltpu.SemaphoreType.DMA

    def kernel(a, b, c, d, result, *refs):
        new_bufs, old_bufs, refs = refs[:local_experts], refs[local_experts : 2 * local_experts], refs[2 * local_experts :]
        push_kernel(sizes, a, b, c, d, result, new_bufs, old_bufs, *refs[:7], refs[7:])

    return pl.pallas_call(
        kernel,
        name="push",
        out_shape=pltpu.VMEM((2, slots, ROWS, BLK), jnp.bfloat16),
        in_specs=[
            pl.BlockSpec(memory_space=pltpu.HBM),
            pl.BlockSpec(memory_space=pltpu.HBM),
            pl.BlockSpec(memory_space=pltpu.HBM),
            pl.BlockSpec(memory_space=pltpu.HBM),
        ],
        out_specs=pl.BlockSpec(memory_space=pltpu.VMEM),
        scratch_shapes=[
            *[pltpu.VMEM(trained.shape[1:], jnp.float32) for _ in range(local_experts)],
            *[pltpu.VMEM(snapshot.shape[1:], jnp.bfloat16) for _ in range(local_experts)],
            pltpu.SMEM(changed.shape, jnp.int32),
            pltpu.SMEM(placement.shape, jnp.int32),
            pltpu.VMEM((BLK, 2 * BLK), jnp.bfloat16),
            pltpu.VMEM((slots, ROWS, BLK), jnp.bfloat16),
            pltpu.VMEM((local_experts, ROWS, BLK), jnp.bfloat16),
            pltpu.VMEM((slots, ROWS, BLK), jnp.bfloat16),
            pltpu.VMEM((slots, ROWS, BLK), jnp.bfloat16),
            dma((2, local_experts)),
            dma((2,)),
            dma,
            dma,
            dma,
            dma((len(PIECES), slots)),
            dma,
            dma((slots,)),
            dma,
            dma,
        ],
        compiler_params=pltpu.CompilerParams(collective_id=0, has_side_effects=True, vmem_limit_bytes=60 * 1024 * 1024),
    )(trained, snapshot, changed, placement)


def spread_kernel(sizes, tiles, out, image, sems):
    tensor_count, group, block_rows = sizes

    def write(z):
        rows = pl.ds(pl.multiple_of(z * block_rows * BLK, BLK), block_rows * BLK)
        return pltpu.make_async_copy(image.at[z], out.at[0, rows, :], sems.at[z])

    @pl.loop(0, tensor_count)
    def _(z):
        for j in range(group):
            index = z * group + j
            spots = []
            for k in range(MOST):
                row = HALF * BLK + (k % HALF) * (META // HALF)
                spots.append(jnp.broadcast_to(tiles[k // HALF, index, row : row + 1, :], (CHUNK, BLK)))
            for first in range(0, BLK, CHUNK):
                values = []
                for k in range(MOST):
                    row = (k % HALF) * BLK + first
                    values.append(tiles[k // HALF, index, row : row + CHUNK, :])
                for b in range(block_rows):
                    value = jnp.zeros((CHUNK, BLK), jnp.bfloat16)
                    for k in range(MOST):
                        value = jnp.where(spots[k] == jnp.bfloat16(b), values[k], value)
                    image[z, b * BLK + first : b * BLK + first + CHUNK, j * BLK : (j + 1) * BLK] = value
        write(z).start()

    @pl.loop(0, tensor_count)
    def _(z):
        write(z).wait()


def spread(tiles, block_rows):
    tensor_count = lax.axis_size("tensor")
    group = tiles.shape[1] // tensor_count
    rows = block_rows * BLK

    def kernel(tiles_ref, out, image, sems):
        spread_kernel((tensor_count, group, block_rows), tiles_ref, out, image, sems)

    return pl.pallas_call(
        kernel,
        name="spread",
        out_shape=jax.ShapeDtypeStruct((1, tensor_count * rows, group * BLK), jnp.bfloat16),
        in_specs=[pl.BlockSpec(memory_space=pltpu.VMEM)],
        out_specs=pl.BlockSpec(memory_space=pl.ANY),
        scratch_shapes=[
            pltpu.VMEM((tensor_count, rows, group * BLK), jnp.bfloat16),
            pltpu.SemaphoreType.DMA((tensor_count,)),
        ],
        compiler_params=pltpu.CompilerParams(vmem_limit_bytes=24 * 1024 * 1024),
    )(tiles)


def body(trained, snapshot, changed, placement):
    local_experts, local_rows, _ = trained.shape
    block_rows = local_rows // BLK
    blocks = (local_experts, block_rows, BLK, BLK)
    tiles = push(trained.reshape(blocks), snapshot.reshape(blocks), changed.transpose(1, 2, 0), placement)
    return spread(tiles, block_rows)


def solution(mesh):
    in_specs = (
        P("replica", "tensor", "expert"),
        P("replica", "tensor", "expert"),
        P("replica", "tensor", "expert"),
        P(),
    )
    out_specs = P("expert", None, "tensor")
    return jax.shard_map(body, mesh=mesh, in_specs=in_specs, out_specs=out_specs, check_vma=False)
```
